256 devices in a mesh: lat: 16 (over y_hi, z), lon: 16 (over x, y_lo, core).
Axes of the slice: x: 4, y: 4 (y_hi: 2, y_lo: 2; y = y_hi * 2 + y_lo), z: 8, core: 2. Of those that a mesh axis runs over, the one named last changes fastest.
Arguments:
- predicted_state: bfloat16 [222, 640, 2048], P(None, 'lat', 'lon'), may hold values from -30 to 30
- observed_state: bfloat16 [222, 640, 2048], P(None, 'lat', 'lon'), may hold values from -30 to 30
- longterm_average_state: bfloat16 [222, 640, 2048], P(None, 'lat', 'lon'), may hold values from -30 to 30
Outputs:
- blurred_mismatch_map: bfloat16 [222, 640, 2048], P(None, 'lat', 'lon')
- quadratic_mean_mistake: float32 [222], replicated
- pattern_agreement: float32 [222], replicated
The draws below stay inside these ranges and needn't reach their ends.
All inputs are finite; a program needn't handle non-finite values.
Results may differ from the reference program's by a relative error of at most 0.00155.
Values may be sent and summed in bfloat16 or wider, within the bound.
A program may use at most 128 MiB of HBM per device.

```python
import jax
import jax.numpy as jnp
from jax import lax

FIELDS = 222
NLAT = 640
NLON = 2048


def joint_fields(key):
    base = jax.random.fold_in(key, 11)
    key_climate, key_anomaly, random_seed_mistake = jax.random.split(base, 3)
    mesh_dimensions = (FIELDS, NLAT, NLON)
    lat_frac = jnp.arange(NLAT, dtype=jnp.float32) / (NLAT - 1)
    lon_frac = jnp.arange(NLON, dtype=jnp.float32) / (NLON - 1)
    anomaly_strength = (1.0 + 2.0 * lat_frac)[:, None] * (1.0 + 2.0 * lon_frac)[None, :] / 3.0
    normal_reference_state = 2.0 * jax.random.normal(key_climate, mesh_dimensions, dtype=jnp.float32)
    anomaly = jax.random.normal(key_anomaly, mesh_dimensions, dtype=jnp.float32)
    prediction_mismatch = 0.7 * jax.random.normal(random_seed_mistake, mesh_dimensions, dtype=jnp.float32)
    observed_state = normal_reference_state + anomaly
    predicted_state = observed_state + prediction_mismatch * anomaly_strength
    return (jnp.clip(predicted_state, -30.0, 30.0), jnp.clip(observed_state, -30.0, 30.0), jnp.clip(normal_reference_state, -30.0, 30.0))


def draw_predicted_state(key, part):
    return joint_fields(key)[0].astype(jnp.bfloat16)


def draw_observed_state(key, part):
    return joint_fields(key)[1].astype(jnp.bfloat16)


def draw_longterm_average_state(key, part):
    return joint_fields(key)[2].astype(jnp.bfloat16)


def setup_inputs(seed: int = 0) -> dict:
    seeds = jax.random.split(jax.random.key(seed), 4)
    predicted_state = draw_predicted_state(jax.random.fold_in(seeds[3], 71), 0)
    observed_state = draw_observed_state(jax.random.fold_in(seeds[3], 71), 0)
    longterm_average_state = draw_longterm_average_state(jax.random.fold_in(seeds[3], 71), 0)
    return dict(predicted_state=predicted_state, observed_state=observed_state, longterm_average_state=longterm_average_state)


epsilon = 1e-06

def finish(running_accumulations, grid_cells):
    mean_fcst = running_accumulations[1] / grid_cells
    mean_true = running_accumulations[2] / grid_cells
    variance_fcst = running_accumulations[3] / grid_cells - mean_fcst * mean_fcst
    variance_true = running_accumulations[4] / grid_cells - mean_true * mean_true
    covariance = running_accumulations[5] / grid_cells - mean_fcst * mean_true
    quadratic_mean_mistake = jnp.sqrt(running_accumulations[0] / grid_cells)
    pattern_agreement = covariance / jnp.sqrt((variance_fcst + epsilon) * (variance_true + epsilon))
    return (quadratic_mean_mistake, pattern_agreement)

def reference(predicted_state, observed_state, longterm_average_state):
    parallel_overall_accumulated = predicted_state.shape[1]
    meridian_accumulated = predicted_state.shape[2]
    row_index = jnp.arange(parallel_overall_accumulated, dtype=jnp.int32)
    all_rows = jnp.arange(parallel_overall_accumulated, dtype=jnp.float32)
    cosine = jnp.cos(jnp.pi * (0.5 - all_rows / (parallel_overall_accumulated - 1)))
    cosine_factor_vector = (cosine / jnp.mean(cosine))[:, None]
    row_count = 3.0 - (row_index == 0).astype(jnp.float32) - (row_index == parallel_overall_accumulated - 1).astype(jnp.float32)
    divisor = (3.0 * row_count)[:, None]

    def smooth(member):
        padded = jnp.pad(member, ((1, 1), (0, 0)))
        vertical = padded[:-2] + padded[1:-1] + padded[2:]
        horizontal = jnp.roll(vertical, 1, 1) + vertical + jnp.roll(vertical, -1, 1)
        return horizontal / divisor

    def lone_variable_entry(members):
        normal_reference_state = members[2].astype(jnp.float32)
        averaged_prediction = smooth(members[0].astype(jnp.float32) - normal_reference_state)
        averaged_observation = smooth(members[1].astype(jnp.float32) - normal_reference_state)
        prediction_mismatch = averaged_prediction - averaged_observation
        running_accumulations = jnp.stack([jnp.sum(cosine_factor_vector * prediction_mismatch * prediction_mismatch), jnp.sum(cosine_factor_vector * averaged_prediction), jnp.sum(cosine_factor_vector * averaged_observation), jnp.sum(cosine_factor_vector * averaged_prediction * averaged_prediction), jnp.sum(cosine_factor_vector * averaged_observation * averaged_observation), jnp.sum(cosine_factor_vector * averaged_prediction * averaged_observation)])
        return (prediction_mismatch.astype(jnp.bfloat16), running_accumulations)
    blurred_mismatch_map, running_accumulations = lax.map(lone_variable_entry, (predicted_state, observed_state, longterm_average_state))
    quadratic_mean_mistake, pattern_agreement = finish(jnp.transpose(running_accumulations), float(parallel_overall_accumulated * meridian_accumulated))
    return (blurred_mismatch_map, quadratic_mean_mistake, pattern_agreement)
```

```python
import functools
import math

import jax
import jax.numpy as jnp
import numpy as np
from jax import lax
from jax.experimental import pallas as pl
from jax.experimental.pallas import tpu as pltpu
from jax.sharding import PartitionSpec as P

epsilon = 1e-06
MESH = pl.DeviceIdType.MESH
F32 = jnp.float32
LANES = 128
CHUNKS = 8


def mean_cosine(rows):
    i = np.arange(rows, dtype=np.float64)
    return float(np.mean(np.cos(np.pi * (0.5 - i / (rows - 1)))))


def kernel(
    nlat, nlon, fields, rows, bounds,
    p_hbm, o_hbm, c_hbm,
    out_ref, rmse_ref, acc_ref,
    p, o, c, nat, slab, diff, halo, side_out, side_in, weight, sums, part, got, tot,
    in_sem, lat_send, lat_recv, lon_send, lon_recv, cor_send, cor_recv, red_send, red_recv,
):
    lat = lax.axis_index("lat")
    lon = lax.axis_index("lon")
    up = lax.rem(lat + nlat - 1, nlat)
    down = lax.rem(lat + 1, nlat)
    left = lax.rem(lon + nlon - 1, nlon)
    right = lax.rem(lon + 1, nlon)
    tiles = slab.shape[1]
    total_rows = nlat * rows

    loads = []
    for k, (lo, hi) in enumerate(bounds):
        span = pl.ds(lo * rows, (hi - lo) * rows)
        group = [
            pltpu.make_async_copy(src.at[span, :], dst.at[span, :], in_sem.at[k, n])
            for n, (src, dst) in enumerate(((p_hbm, p), (o_hbm, o), (c_hbm, c)))
        ]
        for copy in group:
            copy.start()
        loads.append(group)

    barrier = pltpu.get_barrier_semaphore()

    def greet_lon(k, carry):
        pl.semaphore_signal(
            barrier, inc=1, device_id=(lat, lax.rem(lon + k, nlon)), device_id_type=MESH
        )
        return carry

    def greet_lat(k, carry):
        pl.semaphore_signal(
            barrier, inc=1, device_id=(lax.rem(lat + k, nlat), lon), device_id_type=MESH
        )
        return carry

    corners = ((up, left), (up, right), (down, left), (down, right))
    for peer in corners:
        pl.semaphore_signal(barrier, inc=1, device_id=peer, device_id_type=MESH)
    lax.fori_loop(1, nlon, greet_lon, 0)
    lax.fori_loop(1, nlat, greet_lat, 0)

    row = (lax.broadcasted_iota(jnp.int32, (rows, 8, LANES), 0) + lat * rows).astype(F32)
    cosine = jnp.cos(jnp.pi * (0.5 - row / (total_rows - 1)))
    weight[...] = cosine * (1.0 / mean_cosine(total_rows))
    north = jnp.where(lat == 0, 1.5, 1.0).astype(F32)
    south = jnp.where(lat == nlat - 1, 1.5, 1.0).astype(F32)
    north_in = jnp.where(lat == 0, 0.0, 1.0).astype(F32)
    south_in = jnp.where(lat == nlat - 1, 0.0, 1.0).astype(F32)

    padded = tiles * LANES * rows
    if padded > fields * rows:
        for a in range(2):
            nat[a, fields * rows :, :] = jnp.zeros((padded - fields * rows, LANES), F32)
    step = 2 * rows
    for k, (lo, hi) in enumerate(bounds):
        for copy in loads[k]:
            copy.wait()

        def subtract(i, carry):
            span = pl.ds(pl.multiple_of(i * step, 16), step)
            normal = c[span, :].astype(F32)
            nat[0, span, :] = p[span, :].astype(F32) - normal
            nat[1, span, :] = o[span, :].astype(F32) - normal
            return carry

        lax.fori_loop(lo // 2, hi // 2, subtract, 0)

    def turn(r):
        for a in range(2):
            for j in range(tiles):
                x = nat[a, pl.ds(j * LANES * rows + r, LANES, stride=rows), :]
                slab[a, j, r, pl.ds(8, LANES), :] = x.T

    turn(0)
    turn(rows - 1)
    pl.semaphore_wait(barrier, nlon - 1 + nlat - 1 + 4)
    lat_copies = []
    for d, (peer, r) in enumerate(((up, 0), (down, rows - 1))):
        copy = pltpu.make_async_remote_copy(
            src_ref=slab.at[:, :, r, pl.ds(8, LANES), :],
            dst_ref=halo.at[1 - d, :, :, pl.ds(8, LANES), :],
            send_sem=lat_send.at[d],
            recv_sem=lat_recv.at[1 - d],
            device_id=(peer, lon),
            device_id_type=MESH,
        )
        copy.start()
        lat_copies.append(copy)

    def turn_rest(r, carry):
        turn(r)
        return carry

    lax.fori_loop(1, rows - 1, turn_rest, 0)

    for s, column in enumerate((8, 7 + LANES)):
        for a in range(2):
            for j in range(tiles):
                side_out[s, :, a * tiles + j, :] = slab[a, j, :, column, :]
    lon_copies = []
    for s, peer in enumerate((left, right)):
        copy = pltpu.make_async_remote_copy(
            src_ref=side_out.at[s],
            dst_ref=side_in.at[1 - s, pl.ds(1, rows)],
            send_sem=lon_send.at[s],
            recv_sem=lon_recv.at[1 - s],
            device_id=(lat, peer),
            device_id_type=MESH,
        )
        copy.start()
        lon_copies.append(copy)
    cor_copies = []
    for n, peer in enumerate(corners):
        v, s = n // 2, n % 2
        copy = pltpu.make_async_remote_copy(
            src_ref=side_out.at[s, 0 if v == 0 else rows - 1],
            dst_ref=side_in.at[1 - s, rows + 1 if v == 0 else 0],
            send_sem=cor_send.at[n],
            recv_sem=cor_recv.at[3 - n],
            device_id=peer,
            device_id_type=MESH,
        )
        copy.start()
        cor_copies.append(copy)

    def across(ref, index, g):
        low = ref[(*index, pl.ds(g * 8 + 7, 8), slice(None))]
        mid = ref[(*index, pl.ds(pl.multiple_of(g * 8 + 8, 8), 8), slice(None))]
        high = ref[(*index, pl.ds(g * 8 + 9, 8), slice(None))]
        return low + mid + high

    def account(acc, j, r, g, fcst, true):
        s0, s1, s2, s3, s4, s5 = acc
        w = weight[r]
        delta = fcst - true
        diff[j, r, pl.ds(pl.multiple_of(g * 8, 8), 8), :] = delta
        wf = w * fcst
        wt = w * true
        return (
            s0 + (w * delta) * delta,
            s1 + wf,
            s2 + wt,
            s3 + wf * fcst,
            s4 + wt * true,
            s5 + wf * true,
        )

    def inner(j, g, acc):
        fa, ta = across(slab, (0, j, 0), g), across(slab, (1, j, 0), g)
        fb, tb = across(slab, (0, j, 1), g), across(slab, (1, j, 1), g)
        for r in range(1, rows - 1):
            fc, tc = across(slab, (0, j, r + 1), g), across(slab, (1, j, r + 1), g)
            acc = account(acc, j, r, g, fa + fb + fc, ta + tb + tc)
            fa, fb, ta, tb = fb, fc, tb, tc
        return acc

    def outer(j, g, acc):
        both = []
        for a in range(2):
            above = across(halo, (0, a, j), g) * north_in
            x = above + across(slab, (a, j, 0), g) + across(slab, (a, j, 1), g)
            both.append(x * north)
        acc = account(acc, j, 0, g, *both)
        both = []
        for a in range(2):
            below = across(halo, (1, a, j), g) * south_in
            x = across(slab, (a, j, rows - 2), g) + across(slab, (a, j, rows - 1), g) + below
            both.append(x * south)
        return account(acc, j, rows - 1, g, *both)

    groups = LANES // 8
    zero = tuple(jnp.zeros((8, LANES), F32) for _ in range(6))
    accs = [
        lax.fori_loop(1, groups - 1, lambda g, acc, j=j: inner(j, g, acc), zero)
        for j in range(tiles)
    ]

    for copy in lon_copies:
        copy.wait_recv()
    for s, column in enumerate((7, 8 + LANES)):
        for a in range(2):
            for j in range(tiles):
                slab[a, j, :, column, :] = side_in[s, pl.ds(1, rows), a * tiles + j, :]
    for j in range(tiles):
        accs[j] = lax.fori_loop(
            0, 2, lambda g, acc, j=j: inner(j, g * (groups - 1), acc), accs[j]
        )

    for copy in lat_copies:
        copy.wait_recv()
    for copy in cor_copies:
        copy.wait_recv()
    for s, column in enumerate((7, 8 + LANES)):
        for v, r in enumerate((0, rows + 1)):
            for a in range(2):
                for j in range(tiles):
                    halo[v, a, j, pl.ds(column, 1), :] = side_in[s, r, pl.ds(a * tiles + j, 1), :]
    for j in range(tiles):
        accs[j] = lax.fori_loop(0, groups, lambda g, acc, j=j: outer(j, g, acc), accs[j])

    for j in range(tiles):
        for n in range(6):
            sums[0, j, pl.ds(n, 1), :] = jnp.sum(accs[j][n], axis=0, keepdims=True)
        sums[0, j, pl.ds(6, 2), :] = jnp.zeros((2, LANES), F32)

    def exchange(stage, me, count, peer_of):
        def send(k):
            return pltpu.make_async_remote_copy(
                src_ref=sums.at[stage],
                dst_ref=got.at[stage, me],
                send_sem=red_send.at[stage, k],
                recv_sem=red_recv.at[stage, me],
                device_id=peer_of(lax.rem(me + k, count)),
                device_id_type=MESH,
            )

        def receive(k):
            who = lax.rem(me + k, count)
            return pltpu.make_async_remote_copy(
                src_ref=sums.at[stage],
                dst_ref=got.at[stage, who],
                send_sem=red_send.at[stage, k],
                recv_sem=red_recv.at[stage, who],
                device_id=peer_of(who),
                device_id_type=MESH,
            )

        def start(k, carry):
            send(k).start()
            return carry

        def finish(k, carry):
            receive(k).wait_recv()
            return carry

        def drain(k, carry):
            send(k).wait_send()
            return carry

        lax.fori_loop(1, count, start, 0)
        got[stage, me] = sums[stage]
        return (
            lambda: lax.fori_loop(1, count, finish, 0),
            lambda: lax.fori_loop(1, count, drain, 0),
        )

    def added(stage, count):
        x = got[stage, 0]
        for k in range(1, count):
            x = x + got[stage, k]
        return x

    arrive0, drain0 = exchange(0, lon, nlon, lambda q: (lat, q))

    def turn_back(r, carry):
        for j in range(tiles):
            x = diff[j, r] * (1.0 / 9.0)
            nat[0, pl.ds(j * LANES * rows + r, LANES, stride=rows), :] = x.T
        return carry

    lax.fori_loop(0, rows // 2, turn_back, 0)
    arrive0()
    sums[1] = added(0, nlon)
    arrive1, drain1 = exchange(1, lat, nlat, lambda q: (q, lon))
    lax.fori_loop(rows // 2, rows, turn_back, 0)

    def narrow(i, carry):
        span = pl.ds(pl.multiple_of(i * step, 16), step)
        out_ref[span, :] = nat[0, span, :].astype(jnp.bfloat16)
        return carry

    lax.fori_loop(0, fields // 2, narrow, 0)
    arrive1()
    tot[...] = added(1, nlat)

    cells = float(total_rows * nlon * LANES)
    for j in range(tiles):
        width = min(LANES, fields - j * LANES)
        s = [tot[j, pl.ds(n, 1), :] for n in range(6)]
        one, two = 1.0 / (9.0 * cells), 1.0 / (81.0 * cells)
        mf, mt = s[1] * one, s[2] * one
        vf = s[3] * two - mf * mf
        vt = s[4] * two - mt * mt
        cv = s[5] * two - mf * mt
        span = pl.ds(j * LANES, width)
        rmse_ref[:, span] = jnp.sqrt(s[0] * two)[:, :width]
        acc_ref[:, span] = (cv / jnp.sqrt((vf + epsilon) * (vt + epsilon)))[:, :width]

    for copy in lat_copies + lon_copies + cor_copies:
        copy.wait_send()
    drain0()
    drain1()


def local(nlat, nlon, predicted_state, observed_state, longterm_average_state):
    fields, rows, columns = predicted_state.shape
    tiles = pl.cdiv(fields, LANES)
    flat = [
        x.reshape(fields * rows, columns)
        for x in (predicted_state, observed_state, longterm_average_state)
    ]
    edges = [2 * (fields // 2 * k // CHUNKS) for k in range(CHUNKS + 1)]
    bounds = tuple((lo, hi) for lo, hi in zip(edges[:-1], edges[1:]) if hi > lo)
    in_vmem = pltpu.VMEM((fields * rows, columns), jnp.bfloat16)
    blurred, rmse, acc = pl.pallas_call(
        functools.partial(kernel, nlat, nlon, fields, rows, bounds),
        out_shape=(
            jax.ShapeDtypeStruct((fields * rows, columns), jnp.bfloat16),
            jax.ShapeDtypeStruct((1, fields), F32),
            jax.ShapeDtypeStruct((1, fields), F32),
        ),
        in_specs=[pl.BlockSpec(memory_space=pltpu.HBM)] * 3,
        out_specs=[pl.BlockSpec(memory_space=pltpu.VMEM)] * 3,
        scratch_shapes=[
            in_vmem, in_vmem, in_vmem,
            pltpu.VMEM((2, tiles * LANES * rows, LANES), F32),
            pltpu.VMEM((2, tiles, rows, LANES + 16, LANES), F32),
            pltpu.VMEM((tiles, rows, LANES, LANES), F32),
            pltpu.VMEM((2, 2, tiles, LANES + 16, LANES), F32),
            pltpu.VMEM((2, rows, 2 * tiles, LANES), F32),
            pltpu.VMEM((2, rows + 2, 2 * tiles, LANES), F32),
            pltpu.VMEM((rows, 8, LANES), F32),
            pltpu.VMEM((2, tiles, 8, LANES), F32),
            pltpu.VMEM((8, LANES), F32),
            pltpu.VMEM((2, max(nlat, nlon), tiles, 8, LANES), F32),
            pltpu.VMEM((tiles, 8, LANES), F32),
            pltpu.SemaphoreType.DMA((CHUNKS, 3)),
            pltpu.SemaphoreType.DMA((2,)),
            pltpu.SemaphoreType.DMA((2,)),
            pltpu.SemaphoreType.DMA((2,)),
            pltpu.SemaphoreType.DMA((2,)),
            pltpu.SemaphoreType.DMA((4,)),
            pltpu.SemaphoreType.DMA((4,)),
            pltpu.SemaphoreType.DMA((2, max(nlat, nlon))),
            pltpu.SemaphoreType.DMA((2, max(nlat, nlon))),
        ],
        compiler_params=pltpu.CompilerParams(
            collective_id=0, has_side_effects=True, vmem_limit_bytes=56 * 1024 * 1024
        ),
    )(*flat)
    return (
        blurred.reshape(fields, rows, columns),
        rmse.reshape(fields),
        acc.reshape(fields),
    )


def solution(mesh):
    placed = (P(None, "lat", "lon"), P(None, "lat", "lon"), P(None, "lat", "lon"))
    return jax.shard_map(
        functools.partial(local, mesh.shape["lat"], mesh.shape["lon"]),
        mesh=mesh,
        in_specs=placed,
        out_specs=(P(None, "lat", "lon"), P(), P()),
        check_vma=False,
    )
```

```python
import functools
import math

import jax
import jax.numpy as jnp
import numpy as np
from jax import lax
from jax.experimental import pallas as pl
from jax.experimental.pallas import tpu as pltpu
from jax.sharding import PartitionSpec as P

epsilon = 1e-06
MESH = pl.DeviceIdType.MESH
F32 = jnp.float32
LANES = 128
STEP = 8
CHUNK = 32


def mean_cosine(rows):
    i = np.arange(rows, dtype=np.float64)
    return float(np.mean(np.cos(np.pi * (0.5 - i / (rows - 1)))))


def kernel(
    nlat, nlon, fields, rows, bounds,
    p_hbm, o_hbm, c_hbm,
    out_ref, rmse_ref, acc_ref,
    p, o, c, nat, slab, diff, halo, edge, edge_out, edge_in, side_out, side_in,
    weight, sums, got, tot,
    in_sem, lat_send, lat_recv, lon_send, lon_recv, cor_send, cor_recv, red_send, red_recv,
):
    lat = lax.axis_index("lat")
    lon = lax.axis_index("lon")
    up = lax.rem(lat + nlat - 1, nlat)
    down = lax.rem(lat + 1, nlat)
    left = lax.rem(lon + nlon - 1, nlon)
    right = lax.rem(lon + 1, nlon)
    tiles = slab.shape[1]
    total_rows = nlat * rows

    depth, width = nlat // 2, nlon // 4
    z, y_hi = lax.rem(lat, depth), lat // depth
    core, y_lo, x = lax.rem(lon, 2), lax.rem(lon // 2, 2), lon // 4
    y = y_hi * 2 + y_lo

    def place(px, py, pz, pc):
        return ((py // 2) * depth + pz, (px * 2 + lax.rem(py, 2)) * 2 + pc)

    def ring(a, b, n):
        return min((a - b) % n, (b - a) % n)

    plane = sorted(
        ((dx, dy) for dx in range(width) for dy in range(4) if dx or dy),
        key=lambda q: -ring(q[0], 0, width) - ring(q[1], 0, 4),
    )
    line = sorted(
        ((dz, dc) for dz in range(depth) for dc in range(2) if dz or dc),
        key=lambda q: -ring(q[0], 0, depth) - 0.5 * q[1],
    )
    plane_peers = []
    for dx, dy in plane:
        px, py = lax.rem(x + dx, width), lax.rem(y + dy, 4)
        plane_peers.append((place(px, py, z, core), px * 4 + py))
    line_peers = []
    for dz, dc in line:
        pz, pc = lax.rem(z + dz, depth), lax.rem(core + dc, 2)
        line_peers.append((place(x, y, pz, pc), pz * 2 + pc))
    corners = ((up, left), (up, right), (down, left), (down, right))
    sides = ((up, lon), (down, lon), (lat, left), (lat, right))

    barrier = pltpu.get_barrier_semaphore()
    greeted = [q[0] for q in line_peers + plane_peers] + list(sides) + list(corners)
    for peer in greeted:
        pl.semaphore_signal(barrier, inc=1, device_id=peer, device_id_type=MESH)

    loads = []
    for k, (lo, hi) in enumerate(bounds):
        span = pl.ds(lo * rows, (hi - lo) * rows)
        group = [
            pltpu.make_async_copy(src.at[span, :], dst.at[span, :], in_sem.at[k, n])
            for n, (src, dst) in enumerate(((p_hbm, p), (o_hbm, o), (c_hbm, c)))
        ]
        for copy in group:
            copy.start()
        loads.append(group)

    row = (lax.broadcasted_iota(jnp.int32, (rows, 8, LANES), 0) + lat * rows).astype(F32)
    cosine = jnp.cos(jnp.pi * (0.5 - row / (total_rows - 1)))
    weight[...] = cosine * (1.0 / mean_cosine(total_rows))
    north = jnp.where(lat == 0, 1.5, 1.0).astype(F32)
    south = jnp.where(lat == nlat - 1, 1.5, 1.0).astype(F32)
    north_in = jnp.where(lat == 0, 0.0, 1.0).astype(F32)
    south_in = jnp.where(lat == nlat - 1, 0.0, 1.0).astype(F32)

    padded = tiles * LANES * rows
    if padded > fields * rows:
        for a in range(2):
            nat[a, fields * rows :, :] = jnp.zeros((padded - fields * rows, LANES), F32)
    edge[:, :, fields:, :] = jnp.zeros((2, 3, edge.shape[2] - fields, LANES), F32)

    def subtract(first, count):
        start = first * rows
        if not isinstance(start, int):
            start = pl.multiple_of(start, 16)
        span = pl.ds(start, count * rows)
        three = [src[span, :].astype(F32) for src in (p, o, c)]
        nat[0, span, :] = three[0] - three[2]
        nat[1, span, :] = three[1] - three[2]
        for n in range(3):
            for q in range(count):
                for v, r in enumerate((0, rows - 1)):
                    at = q * rows + r
                    edge[v, n, pl.ds(first + q, 1), :] = three[n][at : at + 1, :]

    def subtract_chunk(k):
        lo, hi = bounds[k]
        for copy in loads[k]:
            copy.wait()
        whole = (hi - lo) // STEP

        def body(i, carry):
            subtract(lo + i * STEP, STEP)
            return carry

        lax.fori_loop(0, whole, body, 0)
        if lo + whole * STEP < hi:
            subtract(lo + whole * STEP, hi - lo - whole * STEP)

    def turn(j, r):
        for a in range(2):
            t = nat[a, pl.ds(j * LANES * rows + r, LANES, stride=rows), :]
            slab[a, j, r, pl.ds(8, LANES), :] = t.T

    def turn_all(j):
        def body(i, carry):
            for k in range(rows // 2):
                turn(j, i * (rows // 2) + k)
            return carry

        lax.fori_loop(0, 2, body, 0)

    for j in range(tiles):
        for k, (lo, hi) in enumerate(bounds):
            if lo // LANES == j:
                subtract_chunk(k)
        if j < tiles - 1:
            turn_all(j)

    for v in range(2):
        for n in range(3):
            edge_out[v, n] = edge[v, n].astype(jnp.bfloat16)
    pl.semaphore_wait(barrier, len(greeted))
    lat_copies = []
    for v, peer in enumerate((up, down)):
        copy = pltpu.make_async_remote_copy(
            src_ref=edge_out.at[v],
            dst_ref=edge_in.at[1 - v],
            send_sem=lat_send.at[v],
            recv_sem=lat_recv.at[1 - v],
            device_id=(peer, lon),
            device_id_type=MESH,
        )
        copy.start()
        lat_copies.append(copy)
    turn_all(tiles - 1)

    for s, column in enumerate((8, 7 + LANES)):
        for a in range(2):
            for j in range(tiles):
                side_out[s, :, a * tiles + j, :] = slab[a, j, :, column, :]
    lon_copies = []
    for s, peer in enumerate((left, right)):
        copy = pltpu.make_async_remote_copy(
            src_ref=side_out.at[s],
            dst_ref=side_in.at[1 - s, pl.ds(1, rows)],
            send_sem=lon_send.at[s],
            recv_sem=lon_recv.at[1 - s],
            device_id=(lat, peer),
            device_id_type=MESH,
        )
        copy.start()
        lon_copies.append(copy)
    cor_copies = []
    for n, peer in enumerate(corners):
        v, s = n // 2, n % 2
        copy = pltpu.make_async_remote_copy(
            src_ref=side_out.at[s, 0 if v == 0 else rows - 1],
            dst_ref=side_in.at[1 - s, rows + 1 if v == 0 else 0],
            send_sem=cor_send.at[n],
            recv_sem=cor_recv.at[3 - n],
            device_id=peer,
            device_id_type=MESH,
        )
        copy.start()
        cor_copies.append(copy)

    def across(ref, index, g):
        low = ref[(*index, pl.ds(g * 8 + 7, 8), slice(None))]
        mid = ref[(*index, pl.ds(pl.multiple_of(g * 8 + 8, 8), 8), slice(None))]
        high = ref[(*index, pl.ds(g * 8 + 9, 8), slice(None))]
        return low + mid + high

    def account(acc, j, r, g, fcst, true):
        s0, s1, s2, s3, s4, s5 = acc
        w = weight[r]
        delta = fcst - true
        diff[j, r, pl.ds(pl.multiple_of(g * 8, 8), 8), :] = delta
        wf = w * fcst
        wt = w * true
        return (
            s0 + (w * delta) * delta,
            s1 + wf,
            s2 + wt,
            s3 + wf * fcst,
            s4 + wt * true,
            s5 + wf * true,
        )

    def inner(j, g, acc):
        fa, ta = across(slab, (0, j, 0), g), across(slab, (1, j, 0), g)
        fb, tb = across(slab, (0, j, 1), g), across(slab, (1, j, 1), g)
        for r in range(1, rows - 1):
            fc, tc = across(slab, (0, j, r + 1), g), across(slab, (1, j, r + 1), g)
            acc = account(acc, j, r, g, fa + fb + fc, ta + tb + tc)
            fa, fb, ta, tb = fb, fc, tb, tc
        return acc

    def outer(j, g, acc):
        both = []
        for a in range(2):
            above = across(halo, (0, a, j), g) * north_in
            x = above + across(slab, (a, j, 0), g) + across(slab, (a, j, 1), g)
            both.append(x * north)
        acc = account(acc, j, 0, g, *both)
        both = []
        for a in range(2):
            below = across(halo, (1, a, j), g) * south_in
            x = across(slab, (a, j, rows - 2), g) + across(slab, (a, j, rows - 1), g) + below
            both.append(x * south)
        return account(acc, j, rows - 1, g, *both)

    groups = LANES // 8
    zero = tuple(jnp.zeros((8, LANES), F32) for _ in range(6))
    accs = [
        lax.fori_loop(1, groups - 1, lambda g, acc, j=j: inner(j, g, acc), zero)
        for j in range(tiles)
    ]

    for copy in lon_copies:
        copy.wait_recv()
    for s, column in enumerate((7, 8 + LANES)):
        for a in range(2):
            for j in range(tiles):
                slab[a, j, :, column, :] = side_in[s, pl.ds(1, rows), a * tiles + j, :]
    for j in range(tiles):
        accs[j] = lax.fori_loop(
            0, 2, lambda g, acc, j=j: inner(j, g * (groups - 1), acc), accs[j]
        )

    for copy in lat_copies:
        copy.wait_recv()
    for v in range(2):
        normal = edge_in[v, 2].astype(F32)
        for a in range(2):
            t = edge_in[v, a].astype(F32) - normal
            for j in range(tiles):
                halo[v, a, j, pl.ds(8, LANES), :] = t[j * LANES : (j + 1) * LANES, :].T
    for copy in cor_copies:
        copy.wait_recv()
    for s, column in enumerate((7, 8 + LANES)):
        for v, r in enumerate((0, rows + 1)):
            for a in range(2):
                for j in range(tiles):
                    halo[v, a, j, pl.ds(column, 1), :] = side_in[s, r, pl.ds(a * tiles + j, 1), :]
    for j in range(tiles):
        accs[j] = lax.fori_loop(0, groups, lambda g, acc, j=j: outer(j, g, acc), accs[j])

    for j in range(tiles):
        for n in range(6):
            sums[0, pl.ds(n * tiles + j, 1), :] = jnp.sum(accs[j][n], axis=0, keepdims=True)

    def exchange(stage, me, peers):
        def copy_of(k, slot):
            return pltpu.make_async_remote_copy(
                src_ref=sums.at[stage],
                dst_ref=got.at[stage, slot],
                send_sem=red_send.at[stage, k],
                recv_sem=red_recv.at[stage, slot],
                device_id=peers[k][0],
                device_id_type=MESH,
            )

        for k in range(len(peers)):
            copy_of(k, me).start()
        got[stage, me] = sums[stage]

        def arrive():
            for k, (_, who) in enumerate(peers):
                copy_of(k, who).wait_recv()

        def drain():
            for k in range(len(peers)):
                copy_of(k, me).wait_send()

        return arrive, drain

    def added(stage, count):
        x = got[stage, 0]
        for k in range(1, count):
            x = x + got[stage, k]
        return x

    arrive0, drain0 = exchange(0, x * 4 + y, plane_peers)

    def turn_back(r, carry):
        for j in range(tiles):
            t = diff[j, r] * (1.0 / 9.0)
            nat[0, pl.ds(j * LANES * rows + r, LANES, stride=rows), :] = t.T
        return carry

    lax.fori_loop(0, rows // 2, turn_back, 0)
    arrive0()
    sums[1] = added(0, len(plane_peers) + 1)
    arrive1, drain1 = exchange(1, z * 2 + core, line_peers)
    lax.fori_loop(rows // 2, rows, turn_back, 0)

    def narrow(start, count):
        span = pl.ds(start, count * rows)
        out_ref[span, :] = nat[0, span, :].astype(jnp.bfloat16)

    def narrow_step(i, carry):
        narrow(pl.multiple_of(i * (STEP * rows), 16), STEP)
        return carry

    lax.fori_loop(0, fields // STEP, narrow_step, 0)
    if fields % STEP:
        narrow(fields // STEP * STEP * rows, fields % STEP)
    arrive1()
    tot[...] = added(1, len(line_peers) + 1)

    cells = float(total_rows * nlon * LANES)
    s = [tot[pl.ds(n * tiles, tiles), :] for n in range(6)]
    one, two = 1.0 / (9.0 * cells), 1.0 / (81.0 * cells)
    mf, mt = s[1] * one, s[2] * one
    vf = s[3] * two - mf * mf
    vt = s[4] * two - mt * mt
    cv = s[5] * two - mf * mt
    rmse = jnp.sqrt(s[0] * two)
    acc = cv / jnp.sqrt((vf + epsilon) * (vt + epsilon))
    for j in range(tiles):
        width_j = min(LANES, fields - j * LANES)
        span = pl.ds(j * LANES, width_j)
        rmse_ref[:, span] = rmse[j : j + 1, :width_j]
        acc_ref[:, span] = acc[j : j + 1, :width_j]

    for copy in lat_copies + lon_copies + cor_copies:
        copy.wait_send()
    drain0()
    drain1()


def local(nlat, nlon, predicted_state, observed_state, longterm_average_state):
    fields, rows, columns = predicted_state.shape
    tiles = pl.cdiv(fields, LANES)
    flat = [
        x.reshape(fields * rows, columns)
        for x in (predicted_state, observed_state, longterm_average_state)
    ]
    edges = list(range(0, fields, CHUNK)) + [fields]
    bounds = tuple(zip(edges[:-1], edges[1:]))
    field_rows = tiles * LANES
    group = max(nlat, nlon)
    in_vmem = pltpu.VMEM((fields * rows, columns), jnp.bfloat16)
    blurred, rmse, acc = pl.pallas_call(
        functools.partial(kernel, nlat, nlon, fields, rows, bounds),
        out_shape=(
            jax.ShapeDtypeStruct((fields * rows, columns), jnp.bfloat16),
            jax.ShapeDtypeStruct((1, fields), F32),
            jax.ShapeDtypeStruct((1, fields), F32),
        ),
        in_specs=[pl.BlockSpec(memory_space=pltpu.HBM)] * 3,
        out_specs=[pl.BlockSpec(memory_space=pltpu.VMEM)] * 3,
        scratch_shapes=[
            in_vmem, in_vmem, in_vmem,
            pltpu.VMEM((2, tiles * LANES * rows, LANES), F32),
            pltpu.VMEM((2, tiles, rows, LANES + 16, LANES), F32),
            pltpu.VMEM((tiles, rows, LANES, LANES), F32),
            pltpu.VMEM((2, 2, tiles, LANES + 16, LANES), F32),
            pltpu.VMEM((2, 3, field_rows, LANES), F32),
            pltpu.VMEM((2, 3, field_rows, LANES), jnp.bfloat16),
            pltpu.VMEM((2, 3, field_rows, LANES), jnp.bfloat16),
            pltpu.VMEM((2, rows, 2 * tiles, LANES), F32),
            pltpu.VMEM((2, rows + 2, 2 * tiles, LANES), F32),
            pltpu.VMEM((rows, 8, LANES), F32),
            pltpu.VMEM((2, 6 * tiles, LANES), F32),
            pltpu.VMEM((2, group, 6 * tiles, LANES), F32),
            pltpu.VMEM((6 * tiles, LANES), F32),
            pltpu.SemaphoreType.DMA((len(bounds), 3)),
            pltpu.SemaphoreType.DMA((2,)),
            pltpu.SemaphoreType.DMA((2,)),
            pltpu.SemaphoreType.DMA((2,)),
            pltpu.SemaphoreType.DMA((2,)),
            pltpu.SemaphoreType.DMA((4,)),
            pltpu.SemaphoreType.DMA((4,)),
            pltpu.SemaphoreType.DMA((2, group)),
            pltpu.SemaphoreType.DMA((2, group)),
        ],
        compiler_params=pltpu.CompilerParams(
            collective_id=0, has_side_effects=True, vmem_limit_bytes=50 * 1024 * 1024
        ),
    )(*flat)
    return (
        blurred.reshape(fields, rows, columns),
        rmse.reshape(fields),
        acc.reshape(fields),
    )


def solution(mesh):
    placed = (P(None, "lat", "lon"), P(None, "lat", "lon"), P(None, "lat", "lon"))
    return jax.shard_map(
        functools.partial(local, mesh.shape["lat"], mesh.shape["lon"]),
        mesh=mesh,
        in_specs=placed,
        out_specs=(P(None, "lat", "lon"), P(), P()),
        check_vma=False,
    )
```

```python
import functools
import math

import jax
import jax.numpy as jnp
import numpy as np
from jax import lax
from jax.experimental import pallas as pl
from jax.experimental.pallas import tpu as pltpu
from jax.sharding import PartitionSpec as P

MESH = pl.DeviceIdType.MESH
F32 = jnp.float32
LANES = 128
STEP = 8
AT_ONCE = 7
CHUNK = 64


def mean_cosine(rows):
    i = np.arange(rows, dtype=np.float64)
    return float(np.mean(np.cos(np.pi * (0.5 - i / (rows - 1)))))


def kernel(
    nlat, nlon, fields, rows, bounds,
    p_hbm, o_hbm, c_hbm,
    out_ref, tot_ref,
    p, o, c, nat0, nat1, slab0, slab1, diff, halo, edge, edge_out, edge_in, side_out, side_in,
    pairs, weight, sums, got,
    in_sem, lat_send, lat_recv, lon_send, lon_recv, cor_send, cor_recv, red_send, red_recv,
):
    lat = lax.axis_index("lat")
    lon = lax.axis_index("lon")
    up = lax.rem(lat + nlat - 1, nlat)
    down = lax.rem(lat + 1, nlat)
    left = lax.rem(lon + nlon - 1, nlon)
    right = lax.rem(lon + 1, nlon)
    tiles = 2
    pitch = rows + 1
    nat, slab = (nat0, nat1), (slab0, slab1)
    total_rows = nlat * rows

    loads = []
    for k, (lo, hi) in enumerate(bounds):
        span = pl.ds(lo * rows, (hi - lo) * rows)
        group = [
            pltpu.make_async_copy(src.at[span, :], dst.at[span, :], in_sem.at[k, n])
            for n, (src, dst) in enumerate(((p_hbm, p), (o_hbm, o), (c_hbm, c)))
        ]
        for copy in group:
            copy.start()
        loads.append(group)

    depth, width = nlat // 2, nlon // 4
    z, y_hi = lax.rem(lat, depth), lat // depth
    core, y_lo, x = lax.rem(lon, 2), lax.rem(lon // 2, 2), lon // 4
    y = y_hi * 2 + y_lo

    def place(px, py, pz, pc):
        return ((py // 2) * depth + pz, (px * 2 + lax.rem(py, 2)) * 2 + pc)

    def ring(a, b, n):
        return min((a - b) % n, (b - a) % n)

    plane = sorted(
        ((dx, dy) for dx in range(width) for dy in range(4) if dx or dy),
        key=lambda q: -ring(q[0], 0, width) - ring(q[1], 0, 4),
    )
    line = sorted(
        ((dz, dc) for dz in range(depth) for dc in range(2) if dz or dc),
        key=lambda q: -ring(q[0], 0, depth) - 0.5 * q[1],
    )
    plane_peers = []
    for dx, dy in plane:
        px, py = lax.rem(x + dx, width), lax.rem(y + dy, 4)
        plane_peers.append((place(px, py, z, core), px * 4 + py))
    line_peers = []
    for dz, dc in line:
        pz, pc = lax.rem(z + dz, depth), lax.rem(core + dc, 2)
        line_peers.append((place(x, y, pz, pc), pz * 2 + pc))
    corners = ((up, left), (up, right), (down, left), (down, right))
    sides = ((up, lon), (down, lon), (lat, left), (lat, right))

    barrier = pltpu.get_barrier_semaphore()
    greeted = [q[0] for q in line_peers + plane_peers] + list(sides) + list(corners)
    for peer in greeted:
        pl.semaphore_signal(barrier, inc=1, device_id=peer, device_id_type=MESH)

    row = (lax.broadcasted_iota(jnp.int32, (rows, 8, LANES), 0) + lat * rows).astype(F32)
    cosine = jnp.cos(jnp.pi * (0.5 - row / (total_rows - 1)))
    weight[...] = cosine * (1.0 / mean_cosine(total_rows))
    north = jnp.where(lat == 0, 1.5, 1.0).astype(F32)
    south = jnp.where(lat == nlat - 1, 1.5, 1.0).astype(F32)
    north_in = jnp.where(lat == 0, 0.0, 1.0).astype(F32)
    south_in = jnp.where(lat == nlat - 1, 0.0, 1.0).astype(F32)

    rest = tiles * LANES - fields
    if rest:
        for a in range(2):
            nat1[a, pl.ds((LANES - rest) // 8 * 8 * pitch, (rest + 7) // 8 * 8 * pitch), :] = (
                jnp.zeros(((rest + 7) // 8 * 8 * pitch, LANES), F32)
            )
    if edge.shape[2] > fields:
        edge[:, :, fields:, :] = jnp.zeros((2, 3, edge.shape[2] - fields, LANES), F32)

    def subtract(j, first, count):
        span = pl.ds(pl.multiple_of(first * rows, 16), count * rows)
        three = [src[span, :].astype(F32) for src in (p, o, c)]
        for q in range(count):
            into = pl.ds((first + q - j * LANES) * pitch, rows)
            normal = three[2][q * rows : (q + 1) * rows]
            for a in range(2):
                nat[j][a, into, :] = three[a][q * rows : (q + 1) * rows] - normal
        for n in range(3):
            for q in range(count):
                for v, r in enumerate((0, rows - 1)):
                    at = q * rows + r
                    edge[v, n, pl.ds(first + q, 1), :] = three[n][at : at + 1, :]

    def subtract_chunk(j, lo, hi):
        whole = (hi - lo) // STEP

        def body(i, carry):
            subtract(j, lo + i * STEP, STEP)
            return carry

        lax.fori_loop(0, whole, body, 0)

        def pair(i, carry):
            subtract(j, lo + whole * STEP + 2 * i, 2)
            return carry

        if lo + whole * STEP < hi:
            lax.fori_loop(0, (hi - lo - whole * STEP) // 2, pair, 0)

    def turn(j, r):
        for a in range(2):
            t = nat[j][a, pl.ds(r, LANES, stride=pitch), :]
            slab[j][a, r, pl.ds(8, LANES), :] = t.T

    for k, (lo, hi) in enumerate(bounds):
        if lo >= LANES:
            break
        for copy in loads[k]:
            copy.wait()

        subtract_chunk(0, lo, hi)

    def turn_rows(lo, hi):
        for r in range(lo, hi):
            turn(0, r)

    turn_rows(0, rows // 2)
    for k, (lo, hi) in enumerate(bounds):
        if lo >= LANES:
            for copy in loads[k]:
                copy.wait()
            subtract_chunk(1, lo, hi)

    for v in range(2):
        for n in range(3):
            edge_out[v, n] = edge[v, n].astype(jnp.bfloat16)
    pl.semaphore_wait(barrier, len(greeted))
    lat_copies = []
    for v, peer in enumerate((up, down)):
        copy = pltpu.make_async_remote_copy(
            src_ref=edge_out.at[v],
            dst_ref=edge_in.at[1 - v],
            send_sem=lat_send.at[v],
            recv_sem=lat_recv.at[1 - v],
            device_id=(peer, lon),
            device_id_type=MESH,
        )
        copy.start()
        lat_copies.append(copy)
    turn_rows(rows // 2, rows)

    def send_columns(j):
        copies = []
        for s, peer in enumerate((left, right)):
            column = 8 if s == 0 else 7 + LANES
            for a in range(2):
                side_out[j, s, :, a, :] = slab[j][a, :, column, :]
        for s, peer in enumerate((left, right)):
            copies.append(
                pltpu.make_async_remote_copy(
                    src_ref=side_out.at[j, s],
                    dst_ref=side_in.at[j, 1 - s, pl.ds(1, rows)],
                    send_sem=lon_send.at[j, s],
                    recv_sem=lon_recv.at[j, 1 - s],
                    device_id=(lat, peer),
                    device_id_type=MESH,
                )
            )
        for n, peer in enumerate(corners):
            v, s = n // 2, n % 2
            copies.append(
                pltpu.make_async_remote_copy(
                    src_ref=side_out.at[j, s, 0 if v == 0 else rows - 1],
                    dst_ref=side_in.at[j, 1 - s, rows + 1 if v == 0 else 0],
                    send_sem=cor_send.at[j, n],
                    recv_sem=cor_recv.at[j, 3 - n],
                    device_id=peer,
                    device_id_type=MESH,
                )
            )
        for copy in copies:
            copy.start()
        return copies[:2], copies[2:]

    def take_columns(j):
        for s, column in enumerate((7, 8 + LANES)):
            for a in range(2):
                slab[j][a, :, column, :] = side_in[j, s, pl.ds(1, rows), a, :]

    def across(ref, index, g):
        low = ref[(*index, pl.ds(g * 8 + 7, 8), slice(None))]
        mid = ref[(*index, pl.ds(pl.multiple_of(g * 8 + 8, 8), 8), slice(None))]
        high = ref[(*index, pl.ds(g * 8 + 9, 8), slice(None))]
        return low + mid + high

    def account(acc, j, r, g, fcst, true):
        s0, s1, s2, s3, s4, s5 = acc
        w = weight[r]
        delta = fcst - true
        diff[j, r, pl.ds(pl.multiple_of(g * 8, 8), 8), :] = delta
        wf = w * fcst
        wt = w * true
        return (
            s0 + (w * delta) * delta,
            s1 + wf,
            s2 + wt,
            s3 + wf * fcst,
            s4 + wt * true,
            s5 + wf * true,
        )

    def inner(j, g, acc):
        fa, ta = across(slab[j], (0, 0), g), across(slab[j], (1, 0), g)
        fb, tb = across(slab[j], (0, 1), g), across(slab[j], (1, 1), g)
        at = pl.ds(pl.multiple_of(g * 8, 8), 8)
        pairs[0, 0, j, at, :], pairs[0, 1, j, at, :] = fa + fb, ta + tb
        for r in range(1, rows - 1):
            fc, tc = across(slab[j], (0, r + 1), g), across(slab[j], (1, r + 1), g)
            acc = account(acc, j, r, g, fa + fb + fc, ta + tb + tc)
            fa, fb, ta, tb = fb, fc, tb, tc
        pairs[1, 0, j, at, :], pairs[1, 1, j, at, :] = fa + fb, ta + tb
        return acc

    def outer(j, g, acc):
        at = pl.ds(pl.multiple_of(g * 8, 8), 8)
        for v, (r, inside, scale) in enumerate(
            ((0, north_in, north), (rows - 1, south_in, south))
        ):
            both = [
                (across(halo, (v, a, j), g) * inside + pairs[v, a, j, at, :]) * scale
                for a in range(2)
            ]
            acc = account(acc, j, r, g, *both)
        return acc

    groups = LANES // 8
    zero = tuple(jnp.zeros((8, LANES), F32) for _ in range(6))
    share = pl.cdiv(rows, groups - 2)

    def mixed(i, acc):
        for q in range(AT_ONCE):
            acc = inner(0, i * AT_ONCE + q + 1, acc)
        for k in range(AT_ONCE * share):
            turn(1, jnp.minimum(i * (AT_ONCE * share) + k, rows - 1))
        return acc

    accs = [None, None]
    lon_copies, cor_copies = [None, None], [None, None]
    lon_copies[0], cor_copies[0] = send_columns(0)
    accs[0] = lax.fori_loop(0, (groups - 2) // AT_ONCE, mixed, zero)
    lon_copies[1], cor_copies[1] = send_columns(1)
    accs[1] = lax.fori_loop(1, groups - 1, lambda g, acc: inner(1, g, acc), zero)

    for j in range(tiles):
        for copy in lon_copies[j]:
            copy.wait_recv()
        take_columns(j)
        accs[j] = lax.fori_loop(
            0, 2, lambda g, acc, j=j: inner(j, g * (groups - 1), acc), accs[j]
        )

    for copy in lat_copies:
        copy.wait_recv()
    tail = edge_in.shape[2] - LANES
    for v in range(2):
        normal = edge_in[v, 2].astype(F32)
        for a in range(2):
            t = edge_in[v, a].astype(F32) - normal
            t = jnp.concatenate([t, jnp.zeros((LANES - tail, LANES), F32)], axis=0)
            for j in range(tiles):
                halo[v, a, j, pl.ds(8, LANES), :] = t[j * LANES : (j + 1) * LANES, :].T
    for j in range(tiles):
        for copy in cor_copies[j]:
            copy.wait_recv()
        for s, column in enumerate((7, 8 + LANES)):
            for v, r in enumerate((0, rows + 1)):
                for a in range(2):
                    halo[v, a, j, pl.ds(column, 1), :] = side_in[j, s, r, pl.ds(a, 1), :]

        def outer_four(i, acc, j=j):
            for q in range(4):
                acc = outer(j, i * 4 + q, acc)
            return acc

        accs[j] = lax.fori_loop(0, groups // 4, outer_four, accs[j])

    for j in range(tiles):
        for n in range(6):
            sums[0, pl.ds(n * tiles + j, 1), :] = jnp.sum(accs[j][n], axis=0, keepdims=True)

    def exchange(stage, me, peers):
        def copy_of(k, slot):
            return pltpu.make_async_remote_copy(
                src_ref=sums.at[stage],
                dst_ref=got.at[stage, slot],
                send_sem=red_send.at[stage, k],
                recv_sem=red_recv.at[stage, slot],
                device_id=peers[k][0],
                device_id_type=MESH,
            )

        for k in range(len(peers)):
            copy_of(k, me).start()
        got[stage, me] = sums[stage]

        def arrive():
            for k, (_, who) in enumerate(peers):
                copy_of(k, who).wait_recv()

        def drain():
            for k in range(len(peers)):
                copy_of(k, me).wait_send()

        return arrive, drain

    def added(stage, count):
        x = got[stage, 0]
        for k in range(1, count):
            x = x + got[stage, k]
        return x

    arrive0, drain0 = exchange(0, x * 4 + y, plane_peers)

    def turn_back(r, carry):
        for j in range(tiles):
            t = diff[j, r] * (1.0 / 9.0)
            nat[j][0, pl.ds(r, LANES, stride=pitch), :] = t.T
        return carry

    lax.fori_loop(0, rows // 2, turn_back, 0)
    arrive0()
    sums[1] = added(0, len(plane_peers) + 1)
    arrive1, drain1 = exchange(1, z * 2 + core, line_peers)
    lax.fori_loop(rows // 2, rows, turn_back, 0)

    for j in range(tiles):
        first, count = j * LANES, min(LANES, fields - j * LANES)

        def narrow(i, carry, j=j, first=first):
            for q in range(2):
                f = 2 * i + q
                out_ref[pl.ds(pl.multiple_of((first + f) * rows, 8), rows), :] = nat[j][
                    0, pl.ds(f * pitch, rows), :
                ].astype(jnp.bfloat16)
            return carry

        lax.fori_loop(0, count // 2, narrow, 0)
    arrive1()
    tot_ref[...] = added(1, len(line_peers) + 1)

    for copy in lat_copies + sum(lon_copies + cor_copies, []):
        copy.wait_send()
    drain0()
    drain1()


def finish(cells, fields, map_ref, tot_ref, out_hbm, rmse_hbm, acc_hbm, rmse_ref, acc_ref, sem):
    tiles = 2
    epsilon = 1e-06
    copy = pltpu.make_async_copy(map_ref, out_hbm, sem.at[0])
    copy.start()
    s = [tot_ref[pl.ds(n * tiles, tiles), :] for n in range(6)]
    one, two = 1.0 / (9.0 * cells), 1.0 / (81.0 * cells)
    mf, mt = s[1] * one, s[2] * one
    vf = s[3] * two - mf * mf
    vt = s[4] * two - mt * mt
    cv = s[5] * two - mf * mt
    rmse = jnp.sqrt(s[0] * two)
    acc = cv / jnp.sqrt((vf + epsilon) * (vt + epsilon))
    for j in range(tiles):
        width_j = min(LANES, fields - j * LANES)
        span = pl.ds(j * LANES, width_j)
        rmse_ref[span] = rmse[j, :width_j]
        acc_ref[span] = acc[j, :width_j]
    small = [
        pltpu.make_async_copy(rmse_ref, rmse_hbm, sem.at[1]),
        pltpu.make_async_copy(acc_ref, acc_hbm, sem.at[2]),
    ]
    for other in small:
        other.start()
    for other in [copy, *small]:
        other.wait()


def local(nlat, nlon, predicted_state, observed_state, longterm_average_state):
    fields, rows, columns = predicted_state.shape
    tiles = pl.cdiv(fields, LANES)
    assert tiles == 2 and fields % 2 == 0
    flat = [
        x.reshape(fields * rows, columns)
        for x in (predicted_state, observed_state, longterm_average_state)
    ]
    edges = list(range(0, fields, CHUNK)) + [fields]
    bounds = tuple(zip(edges[:-1], edges[1:]))
    field_rows = pl.cdiv(fields, 16) * 16
    group = max(nlat, nlon)
    in_vmem = pltpu.VMEM((fields * rows, columns), jnp.bfloat16)
    blurred, totals = pl.pallas_call(
        functools.partial(kernel, nlat, nlon, fields, rows, bounds),
        out_shape=(
            jax.ShapeDtypeStruct((fields * rows, columns), jnp.bfloat16),
            jax.ShapeDtypeStruct((6 * tiles, LANES), F32),
        ),
        in_specs=[pl.BlockSpec(memory_space=pltpu.HBM)] * 3,
        out_specs=[pl.BlockSpec(memory_space=pltpu.VMEM)] * 2,
        scratch_shapes=[
            in_vmem, in_vmem, in_vmem,
            pltpu.VMEM((2, LANES * (rows + 1), LANES), F32),
            pltpu.VMEM((2, LANES * (rows + 1), LANES), F32),
            pltpu.VMEM((2, rows, LANES + 16, LANES), F32),
            pltpu.VMEM((2, rows, LANES + 16, LANES), F32),
            pltpu.VMEM((tiles, rows, LANES, LANES), F32),
            pltpu.VMEM((2, 2, tiles, LANES + 16, LANES), F32),
            pltpu.VMEM((2, 3, field_rows, LANES), F32),
            pltpu.VMEM((2, 3, field_rows, LANES), jnp.bfloat16),
            pltpu.VMEM((2, 3, field_rows, LANES), jnp.bfloat16),
            pltpu.VMEM((tiles, 2, rows, 2, LANES), F32),
            pltpu.VMEM((tiles, 2, rows + 2, 2, LANES), F32),
            pltpu.VMEM((2, 2, tiles, LANES, LANES), F32),
            pltpu.VMEM((rows, 8, LANES), F32),
            pltpu.VMEM((2, 6 * tiles, LANES), F32),
            pltpu.VMEM((2, group, 6 * tiles, LANES), F32),
            pltpu.SemaphoreType.DMA((len(bounds), 3)),
            pltpu.SemaphoreType.DMA((2,)),
            pltpu.SemaphoreType.DMA((2,)),
            pltpu.SemaphoreType.DMA((tiles, 2)),
            pltpu.SemaphoreType.DMA((tiles, 2)),
            pltpu.SemaphoreType.DMA((tiles, 4)),
            pltpu.SemaphoreType.DMA((tiles, 4)),
            pltpu.SemaphoreType.DMA((2, group)),
            pltpu.SemaphoreType.DMA((2, group)),
        ],
        compiler_params=pltpu.CompilerParams(
            collective_id=0, has_side_effects=True, vmem_limit_bytes=50 * 1024 * 1024
        ),
    )(*flat)
    blurred, rmse, acc = pl.pallas_call(
        functools.partial(finish, float(nlat * rows * nlon * columns), fields),
        out_shape=(
            jax.ShapeDtypeStruct((fields * rows, columns), jnp.bfloat16),
            jax.ShapeDtypeStruct((fields,), F32),
            jax.ShapeDtypeStruct((fields,), F32),
        ),
        in_specs=[pl.BlockSpec(memory_space=pltpu.VMEM)] * 2,
        out_specs=[pl.BlockSpec(memory_space=pltpu.HBM)] * 3,
        scratch_shapes=[
            pltpu.VMEM((fields,), F32),
            pltpu.VMEM((fields,), F32),
            pltpu.SemaphoreType.DMA((3,)),
        ],
        compiler_params=pltpu.CompilerParams(vmem_limit_bytes=8 * 1024 * 1024),
    )(blurred, totals)
    return (
        blurred.reshape(fields, rows, columns),
        rmse,
        acc,
    )


def solution(mesh):
    placed = (P(None, "lat", "lon"), P(None, "lat", "lon"), P(None, "lat", "lon"))
    return jax.shard_map(
        functools.partial(local, mesh.shape["lat"], mesh.shape["lon"]),
        mesh=mesh,
        in_specs=placed,
        out_specs=(P(None, "lat", "lon"), P(), P()),
        check_vma=False,
    )
```

```python
import functools
import math

import jax
import jax.numpy as jnp
import numpy as np
from jax import lax
from jax.experimental import pallas as pl
from jax.experimental.pallas import tpu as pltpu
from jax.sharding import PartitionSpec as P

MESH = pl.DeviceIdType.MESH
F32 = jnp.float32
LANES = 128
STEP = 8
AT_ONCE = 7
CHUNK = 64


def mean_cosine(rows):
    i = np.arange(rows, dtype=np.float64)
    return float(np.mean(np.cos(np.pi * (0.5 - i / (rows - 1)))))


def kernel(
    nlat, nlon, fields, rows, bounds,
    p_hbm, o_hbm, c_hbm,
    out_ref, tot_ref,
    p, o, c, nat0, nat1, slab0, slab1, diff, halo, edge, edge_out, edge_in, side_out, side_in,
    pairs, weight, sums, got,
    in_sem, lat_send, lat_recv, lon_send, lon_recv, cor_send, cor_recv, red_send, red_recv,
):
    lat = lax.axis_index("lat")
    lon = lax.axis_index("lon")
    up = lax.rem(lat + nlat - 1, nlat)
    down = lax.rem(lat + 1, nlat)
    left = lax.rem(lon + nlon - 1, nlon)
    right = lax.rem(lon + 1, nlon)
    tiles = 2
    pitch = rows + 1
    nat, slab = (nat0, nat1), (slab0, slab1)
    total_rows = nlat * rows

    loads = []
    for k, (lo, hi) in enumerate(bounds):
        span = pl.ds(lo * rows, (hi - lo) * rows)
        group = [
            pltpu.make_async_copy(src.at[span, :], dst.at[span, :], in_sem.at[k, n])
            for n, (src, dst) in enumerate(((p_hbm, p), (o_hbm, o), (c_hbm, c)))
        ]
        for copy in group:
            copy.start()
        loads.append(group)

    depth, width = nlat // 2, nlon // 4
    z, y_hi = lax.rem(lat, depth), lat // depth
    core, y_lo, x = lax.rem(lon, 2), lax.rem(lon // 2, 2), lon // 4
    y = y_hi * 2 + y_lo

    def place(px, py, pz, pc):
        return ((py // 2) * depth + pz, (px * 2 + lax.rem(py, 2)) * 2 + pc)

    def ring(a, b, n):
        return min((a - b) % n, (b - a) % n)

    plane = sorted(
        ((dx, dy) for dx in range(width) for dy in range(4) if dx or dy),
        key=lambda q: -ring(q[0], 0, width) - ring(q[1], 0, 4),
    )
    line = sorted(
        ((dz, dc) for dz in range(depth) for dc in range(2) if dz or dc),
        key=lambda q: -ring(q[0], 0, depth) - 0.5 * q[1],
    )
    plane_peers = []
    for dx, dy in plane:
        px, py = lax.rem(x + dx, width), lax.rem(y + dy, 4)
        plane_peers.append((place(px, py, z, core), px * 4 + py))
    line_peers = []
    for dz, dc in line:
        pz, pc = lax.rem(z + dz, depth), lax.rem(core + dc, 2)
        line_peers.append((place(x, y, pz, pc), pz * 2 + pc))
    corners = ((up, left), (up, right), (down, left), (down, right))
    sides = ((up, lon), (down, lon), (lat, left), (lat, right))

    barrier = pltpu.get_barrier_semaphore()
    greeted = [q[0] for q in line_peers + plane_peers] + list(sides) + list(corners)
    for peer in greeted:
        pl.semaphore_signal(barrier, inc=1, device_id=peer, device_id_type=MESH)

    nought = lon // nlon

    row = (lax.broadcasted_iota(jnp.int32, (rows, 8, LANES), 0) + lat * rows).astype(F32)
    cosine = jnp.cos(jnp.pi * (0.5 - row / (total_rows - 1)))
    weight[...] = cosine * (1.0 / mean_cosine(total_rows))
    north = jnp.where(lat == 0, 1.5, 1.0).astype(F32)
    south = jnp.where(lat == nlat - 1, 1.5, 1.0).astype(F32)
    north_in = jnp.where(lat == 0, 0.0, 1.0).astype(F32)
    south_in = jnp.where(lat == nlat - 1, 0.0, 1.0).astype(F32)

    rest = tiles * LANES - fields
    if rest:
        for a in range(2):
            nat1[a, pl.ds((LANES - rest) // 8 * 8 * pitch, (rest + 7) // 8 * 8 * pitch), :] = (
                jnp.zeros(((rest + 7) // 8 * 8 * pitch, LANES), F32)
            )
    if edge.shape[2] > fields:
        edge[:, :, fields:, :] = jnp.zeros((2, 2, edge.shape[2] - fields, LANES), F32)

    def subtract(j, first, count):
        span = pl.ds(pl.multiple_of(first * rows, 16), count * rows)
        three = [src[span, :].astype(F32) for src in (p, o, c)]
        for q in range(count):
            into = pl.ds((first + q - j * LANES) * pitch, rows)
            normal = three[2][q * rows : (q + 1) * rows]
            for a in range(2):
                nat[j][a, into, :] = three[a][q * rows : (q + 1) * rows] - normal
        for q in range(count):
            for v, r in enumerate((0, rows - 1)):
                at = q * rows + r
                f, t, n = (x[at : at + 1, :] for x in three)
                edge[v, 0, pl.ds(first + q, 1), :] = f - t
                edge[v, 1, pl.ds(first + q, 1), :] = t - n

    def subtract_chunk(j, lo, hi):
        whole = (hi - lo) // STEP

        def body(i, carry):
            subtract(j, lo + i * STEP, STEP)
            return carry

        lax.fori_loop(0, whole, body, 0)

        def pair(i, carry):
            subtract(j, lo + whole * STEP + 2 * i, 2)
            return carry

        if lo + whole * STEP < hi:
            lax.fori_loop(0, (hi - lo - whole * STEP) // 2, pair, 0)

    def turn(j, r):
        for a in range(2):
            t = nat[j][a, pl.ds(r, LANES, stride=pitch), :]
            slab[j][a, r, pl.ds(8, LANES), :] = t.T

    for k, (lo, hi) in enumerate(bounds):
        if lo >= LANES:
            break
        for copy in loads[k]:
            copy.wait()

        subtract_chunk(0, lo, hi)

    def turn_rows(lo, hi):
        for r in range(lo, hi):
            turn(0, r)

    turn_rows(0, rows // 2)
    for k, (lo, hi) in enumerate(bounds):
        if lo >= LANES:
            for copy in loads[k]:
                copy.wait()
            subtract_chunk(1, lo, hi)

    for v in range(2):
        for n in range(2):
            edge_out[v, n] = edge[v, n].astype(jnp.bfloat16)
    pl.semaphore_wait(barrier, len(greeted))
    lat_copies = []
    for v, peer in enumerate((up, down)):
        copy = pltpu.make_async_remote_copy(
            src_ref=edge_out.at[v],
            dst_ref=edge_in.at[1 - v],
            send_sem=lat_send.at[v],
            recv_sem=lat_recv.at[1 - v],
            device_id=(peer, lon),
            device_id_type=MESH,
        )
        copy.start()
        lat_copies.append(copy)
    turn_rows(rows // 2, rows)

    def send_columns(j):
        copies = []
        for s, peer in enumerate((left, right)):
            column = 8 if s == 0 else 7 + LANES
            for a in range(2):
                side_out[j, s, :, a, :] = slab[j][a, :, column, :]
        for s, peer in enumerate((left, right)):
            copies.append(
                pltpu.make_async_remote_copy(
                    src_ref=side_out.at[j, s],
                    dst_ref=side_in.at[j, 1 - s, pl.ds(1, rows)],
                    send_sem=lon_send.at[j, s],
                    recv_sem=lon_recv.at[j, 1 - s],
                    device_id=(lat, peer),
                    device_id_type=MESH,
                )
            )
        for n, peer in enumerate(corners):
            v, s = n // 2, n % 2
            copies.append(
                pltpu.make_async_remote_copy(
                    src_ref=side_out.at[j, s, 0 if v == 0 else rows - 1],
                    dst_ref=side_in.at[j, 1 - s, rows + 1 if v == 0 else 0],
                    send_sem=cor_send.at[j, n],
                    recv_sem=cor_recv.at[j, 3 - n],
                    device_id=peer,
                    device_id_type=MESH,
                )
            )
        for copy in copies:
            copy.start()
        return copies[:2], copies[2:]

    def take_columns(j):
        for s, column in enumerate((7, 8 + LANES)):
            for a in range(2):
                slab[j][a, :, column, :] = side_in[j, s, pl.ds(1, rows), a, :]

    def across(ref, index, g):
        low = ref[(*index, pl.ds(g * 8 + 7, 8), slice(None))]
        mid = ref[(*index, pl.ds(pl.multiple_of(g * 8 + 8, 8), 8), slice(None))]
        high = ref[(*index, pl.ds(g * 8 + 9, 8), slice(None))]
        return low + mid + high

    def account(acc, j, r, g, fcst, true):
        s0, s1, s2, s3, s4, s5 = acc
        w = weight[r]
        delta = fcst - true
        diff[j, r, pl.ds(pl.multiple_of(g * 8, 8), 8), :] = delta
        wf = w * fcst
        wt = w * true
        return (
            s0 + (w * delta) * delta,
            s1 + wf,
            s2 + wt,
            s3 + wf * fcst,
            s4 + wt * true,
            s5 + wf * true,
        )

    def inner(j, g, acc):
        fa, ta = across(slab[j], (0, 0), g), across(slab[j], (1, 0), g)
        fb, tb = across(slab[j], (0, 1), g), across(slab[j], (1, 1), g)
        at = pl.ds(pl.multiple_of(g * 8, 8), 8)
        pairs[0, 0, j, at, :], pairs[0, 1, j, at, :] = fa + fb, ta + tb
        for r in range(1, rows - 1):
            fc, tc = across(slab[j], (0, r + 1), g), across(slab[j], (1, r + 1), g)
            acc = account(acc, j, r, g, fa + fb + fc, ta + tb + tc)
            fa, fb, ta, tb = fb, fc, tb, tc
        pairs[1, 0, j, at, :], pairs[1, 1, j, at, :] = fa + fb, ta + tb
        return acc

    def outer(j, g, acc):
        at = pl.ds(pl.multiple_of(g * 8, 8), 8)
        for v, (r, inside, scale) in enumerate(
            ((0, north_in, north), (rows - 1, south_in, south))
        ):
            both = [
                (across(halo, (v, a, j), g) * inside + pairs[v, a, j, at, :]) * scale
                for a in range(2)
            ]
            acc = account(acc, j, r, g, *both)
        return acc

    groups = LANES // 8
    zero = tuple(jnp.zeros((8, LANES), F32) for _ in range(6))
    share = pl.cdiv(rows, groups - 2)

    def mixed(i, acc):
        for q in range(AT_ONCE):
            acc = inner(0, i * AT_ONCE + q + 1, acc)
        for k in range(AT_ONCE * share):
            turn(1, jnp.minimum(i * (AT_ONCE * share) + k, rows - 1))
        return acc

    accs = [None, None]
    lon_copies, cor_copies = [None, None], [None, None]
    lon_copies[0], cor_copies[0] = send_columns(0)
    accs[0] = lax.fori_loop(0, (groups - 2) // AT_ONCE, mixed, zero)
    lon_copies[1], cor_copies[1] = send_columns(1)
    accs[1] = lax.fori_loop(1, groups - 1, lambda g, acc: inner(1, g, acc), zero)

    def side_groups(j, acc):
        for copy in lon_copies[j]:
            copy.wait_recv()
        take_columns(j)
        return lax.fori_loop(
            0, 2, lambda g, acc: inner(j, g * (groups - 1), acc), acc
        )

    accs[0] = side_groups(0, accs[0])
    for copy in lat_copies:
        copy.wait_recv()
    tail = edge_in.shape[2] - LANES
    for v in range(2):
        true = edge_in[v, 1].astype(F32)
        for a, t in enumerate((edge_in[v, 0].astype(F32) + true, true)):
            t = jnp.concatenate([t, jnp.zeros((LANES - tail, LANES), F32)], axis=0)
            for j in range(tiles):
                halo[v, a, j, pl.ds(8, LANES), :] = t[j * LANES : (j + 1) * LANES, :].T
    for j in range(tiles):

        def outer_seven(i, acc, j=j):
            for q in range(7):
                acc = outer(j, i * 7 + q + 1, acc)
            return acc

        accs[j] = lax.fori_loop(0, (groups - 2) // 7, outer_seven, accs[j])
    accs[1] = side_groups(1, accs[1])
    for j in range(tiles):
        for copy in cor_copies[j]:
            copy.wait_recv()
        for s, column in enumerate((7, 8 + LANES)):
            for v, r in enumerate((0, rows + 1)):
                for a in range(2):
                    halo[v, a, j, pl.ds(column, 1), :] = side_in[j, s, r, pl.ds(a, 1), :]
        for g in (0, groups - 1):
            accs[j] = outer(j, g + nought, accs[j])

    for j in range(tiles):
        for n in range(6):
            sums[0, pl.ds(n * tiles + j, 1), :] = jnp.sum(accs[j][n], axis=0, keepdims=True)

    def exchange(stage, me, peers):
        def copy_of(k, slot):
            return pltpu.make_async_remote_copy(
                src_ref=sums.at[stage],
                dst_ref=got.at[stage, slot],
                send_sem=red_send.at[stage, k],
                recv_sem=red_recv.at[stage, slot],
                device_id=peers[k][0],
                device_id_type=MESH,
            )

        for k in range(len(peers)):
            copy_of(k, me).start()
        got[stage, me] = sums[stage]

        def arrive():
            for k, (_, who) in enumerate(peers):
                copy_of(k, who).wait_recv()

        def drain():
            for k in range(len(peers)):
                copy_of(k, me).wait_send()

        return arrive, drain

    def added(stage, count):
        x = got[stage, 0]
        for k in range(1, count):
            x = x + got[stage, k]
        return x

    arrive0, drain0 = exchange(0, x * 4 + y, plane_peers)

    def turn_back(r, carry):
        for j in range(tiles):
            t = diff[j, r] * (1.0 / 9.0)
            nat[j][0, pl.ds(r, LANES, stride=pitch), :] = t.T
        return carry

    lax.fori_loop(0, rows // 2, turn_back, 0)
    arrive0()
    sums[1] = added(0, len(plane_peers) + 1)
    arrive1, drain1 = exchange(1, z * 2 + core, line_peers)
    lax.fori_loop(rows // 2, rows, turn_back, 0)

    for j in range(tiles):
        first, count = j * LANES, min(LANES, fields - j * LANES)

        def narrow(i, carry, j=j, first=first):
            for q in range(2):
                f = 2 * i + q
                out_ref[pl.ds(pl.multiple_of((first + f) * rows, 8), rows), :] = nat[j][
                    0, pl.ds(f * pitch, rows), :
                ].astype(jnp.bfloat16)
            return carry

        lax.fori_loop(0, count // 2, narrow, 0)
    for copy in lat_copies + sum(lon_copies + cor_copies, []):
        copy.wait_send()
    drain0()
    drain1()
    arrive1()
    tot_ref[...] = added(1, len(line_peers) + 1)


def finish(cells, fields, map_ref, tot_ref, out_hbm, rmse_hbm, acc_hbm, rmse_ref, acc_ref, sem):
    tiles = 2
    epsilon = 1e-06
    copy = pltpu.make_async_copy(map_ref, out_hbm, sem.at[0])
    copy.start()
    s = [tot_ref[pl.ds(n * tiles, tiles), :] for n in range(6)]
    one, two = 1.0 / (9.0 * cells), 1.0 / (81.0 * cells)
    mf, mt = s[1] * one, s[2] * one
    vf = s[3] * two - mf * mf
    vt = s[4] * two - mt * mt
    cv = s[5] * two - mf * mt
    rmse = jnp.sqrt(s[0] * two)
    acc = cv / jnp.sqrt((vf + epsilon) * (vt + epsilon))
    for j in range(tiles):
        width_j = min(LANES, fields - j * LANES)
        span = pl.ds(j * LANES, width_j)
        rmse_ref[span] = rmse[j, :width_j]
        acc_ref[span] = acc[j, :width_j]
    small = [
        pltpu.make_async_copy(rmse_ref, rmse_hbm, sem.at[1]),
        pltpu.make_async_copy(acc_ref, acc_hbm, sem.at[2]),
    ]
    for other in small:
        other.start()
    for other in [copy, *small]:
        other.wait()


def local(nlat, nlon, predicted_state, observed_state, longterm_average_state):
    fields, rows, columns = predicted_state.shape
    tiles = pl.cdiv(fields, LANES)
    assert tiles == 2 and fields % 2 == 0
    flat = [
        x.reshape(fields * rows, columns)
        for x in (predicted_state, observed_state, longterm_average_state)
    ]
    edges = list(range(0, fields, CHUNK)) + [fields]
    bounds = tuple(zip(edges[:-1], edges[1:]))
    field_rows = pl.cdiv(fields, 16) * 16
    group = max(nlat, nlon)
    in_vmem = pltpu.VMEM((fields * rows, columns), jnp.bfloat16)
    blurred, totals = pl.pallas_call(
        functools.partial(kernel, nlat, nlon, fields, rows, bounds),
        out_shape=(
            jax.ShapeDtypeStruct((fields * rows, columns), jnp.bfloat16),
            jax.ShapeDtypeStruct((6 * tiles, LANES), F32),
        ),
        in_specs=[pl.BlockSpec(memory_space=pltpu.HBM)] * 3,
        out_specs=[pl.BlockSpec(memory_space=pltpu.VMEM)] * 2,
        scratch_shapes=[
            in_vmem, in_vmem, in_vmem,
            pltpu.VMEM((2, LANES * (rows + 1), LANES), F32),
            pltpu.VMEM((2, LANES * (rows + 1), LANES), F32),
            pltpu.VMEM((2, rows, LANES + 16, LANES), F32),
            pltpu.VMEM((2, rows, LANES + 16, LANES), F32),
            pltpu.VMEM((tiles, rows, LANES, LANES), F32),
            pltpu.VMEM((2, 2, tiles, LANES + 16, LANES), F32),
            pltpu.VMEM((2, 2, field_rows, LANES), F32),
            pltpu.VMEM((2, 2, field_rows, LANES), jnp.bfloat16),
            pltpu.VMEM((2, 2, field_rows, LANES), jnp.bfloat16),
            pltpu.VMEM((tiles, 2, rows, 2, LANES), F32),
            pltpu.VMEM((tiles, 2, rows + 2, 2, LANES), F32),
            pltpu.VMEM((2, 2, tiles, LANES, LANES), F32),
            pltpu.VMEM((rows, 8, LANES), F32),
            pltpu.VMEM((2, 6 * tiles, LANES), F32),
            pltpu.VMEM((2, group, 6 * tiles, LANES), F32),
            pltpu.SemaphoreType.DMA((len(bounds), 3)),
            pltpu.SemaphoreType.DMA((2,)),
            pltpu.SemaphoreType.DMA((2,)),
            pltpu.SemaphoreType.DMA((tiles, 2)),
            pltpu.SemaphoreType.DMA((tiles, 2)),
            pltpu.SemaphoreType.DMA((tiles, 4)),
            pltpu.SemaphoreType.DMA((tiles, 4)),
            pltpu.SemaphoreType.DMA((2, group)),
            pltpu.SemaphoreType.DMA((2, group)),
        ],
        compiler_params=pltpu.CompilerParams(
            collective_id=0, has_side_effects=True, vmem_limit_bytes=50 * 1024 * 1024
        ),
    )(*flat)
    blurred, rmse, acc = pl.pallas_call(
        functools.partial(finish, float(nlat * rows * nlon * columns), fields),
        out_shape=(
            jax.ShapeDtypeStruct((fields * rows, columns), jnp.bfloat16),
            jax.ShapeDtypeStruct((fields,), F32),
            jax.ShapeDtypeStruct((fields,), F32),
        ),
        in_specs=[pl.BlockSpec(memory_space=pltpu.VMEM)] * 2,
        out_specs=[pl.BlockSpec(memory_space=pltpu.HBM)] * 3,
        scratch_shapes=[
            pltpu.VMEM((fields,), F32),
            pltpu.VMEM((fields,), F32),
            pltpu.SemaphoreType.DMA((3,)),
        ],
        compiler_params=pltpu.CompilerParams(vmem_limit_bytes=8 * 1024 * 1024),
    )(blurred, totals)
    return (
        blurred.reshape(fields, rows, columns),
        rmse,
        acc,
    )


def solution(mesh):
    placed = (P(None, "lat", "lon"), P(None, "lat", "lon"), P(None, "lat", "lon"))
    return jax.shard_map(
        functools.partial(local, mesh.shape["lat"], mesh.shape["lon"]),
        mesh=mesh,
        in_specs=placed,
        out_specs=(P(None, "lat", "lon"), P(), P()),
        check_vma=False,
    )
```

```python
import functools
import math

import jax
import jax.numpy as jnp
import numpy as np
from jax import lax
from jax.experimental import pallas as pl
from jax.experimental.pallas import tpu as pltpu
from jax.sharding import PartitionSpec as P

MESH = pl.DeviceIdType.MESH
F32 = jnp.float32
LANES = 128
STEP = 8
AT_ONCE = 7
CHUNK = 32


def mean_cosine(rows):
    i = np.arange(rows, dtype=np.float64)
    return float(np.mean(np.cos(np.pi * (0.5 - i / (rows - 1)))))


def kernel(
    nlat, nlon, fields, rows, bounds,
    p_hbm, o_hbm, c_hbm,
    out_ref, tot_ref,
    p, o, c, nat0, nat1, slab0, slab1, diff, halo, edge, edge_out, edge_in, side_out, side_in,
    pairs, weight, sums, got,
    in_sem, lat_send, lat_recv, lon_send, lon_recv, cor_send, cor_recv, red_send, red_recv,
):
    lat = lax.axis_index("lat")
    lon = lax.axis_index("lon")
    up = lax.rem(lat + nlat - 1, nlat)
    down = lax.rem(lat + 1, nlat)
    left = lax.rem(lon + nlon - 1, nlon)
    right = lax.rem(lon + 1, nlon)
    tiles = 2
    pitch = rows + 1
    nat, slab = (nat0, nat1), (slab0, slab1)
    total_rows = nlat * rows

    loads = []
    for k, (lo, hi) in enumerate(bounds):
        span = pl.ds(lo * rows, (hi - lo) * rows)
        group = [
            pltpu.make_async_copy(src.at[span, :], dst.at[span, :], in_sem.at[k, n])
            for n, (src, dst) in enumerate(((p_hbm, p), (o_hbm, o), (c_hbm, c)))
        ]
        for copy in group:
            copy.start()
        loads.append(group)

    depth, width = nlat // 2, nlon // 4
    z, y_hi = lax.rem(lat, depth), lat // depth
    core, y_lo, x = lax.rem(lon, 2), lax.rem(lon // 2, 2), lon // 4
    y = y_hi * 2 + y_lo

    def place(px, py, pz, pc):
        return ((py // 2) * depth + pz, (px * 2 + lax.rem(py, 2)) * 2 + pc)

    def ring(a, b, n):
        return min((a - b) % n, (b - a) % n)

    plane = sorted(
        ((dx, dy) for dx in range(width) for dy in range(4) if dx or dy),
        key=lambda q: -ring(q[0], 0, width) - ring(q[1], 0, 4),
    )
    line = sorted(
        ((dz, dc) for dz in range(depth) for dc in range(2) if dz or dc),
        key=lambda q: -ring(q[0], 0, depth) - 0.5 * q[1],
    )
    plane_peers = []
    for dx, dy in plane:
        px, py = lax.rem(x + dx, width), lax.rem(y + dy, 4)
        plane_peers.append((place(px, py, z, core), px * 4 + py))
    line_peers = []
    for dz, dc in line:
        pz, pc = lax.rem(z + dz, depth), lax.rem(core + dc, 2)
        line_peers.append((place(x, y, pz, pc), pz * 2 + pc))
    corners = ((up, left), (up, right), (down, left), (down, right))
    sides = ((up, lon), (down, lon), (lat, left), (lat, right))

    barrier = pltpu.get_barrier_semaphore()
    greeted = [q[0] for q in line_peers + plane_peers] + list(sides) + list(corners)
    for peer in greeted:
        pl.semaphore_signal(barrier, inc=1, device_id=peer, device_id_type=MESH)

    nought = lon // nlon

    row = (lax.broadcasted_iota(jnp.int32, (rows, 8, LANES), 0) + lat * rows).astype(F32)
    cosine = jnp.cos(jnp.pi * (0.5 - row / (total_rows - 1)))
    weight[...] = cosine * (1.0 / mean_cosine(total_rows))
    north = jnp.where(lat == 0, 1.5, 1.0).astype(F32)
    south = jnp.where(lat == nlat - 1, 1.5, 1.0).astype(F32)
    north_in = jnp.where(lat == 0, 0.0, 1.0).astype(F32)
    south_in = jnp.where(lat == nlat - 1, 0.0, 1.0).astype(F32)

    rest = tiles * LANES - fields
    if rest:
        for a in range(2):
            nat1[a, pl.ds((LANES - rest) // 8 * 8 * pitch, (rest + 7) // 8 * 8 * pitch), :] = (
                jnp.zeros(((rest + 7) // 8 * 8 * pitch, LANES), F32)
            )
    if edge.shape[2] > fields:
        edge[:, :, fields:, :] = jnp.zeros((2, 2, edge.shape[2] - fields, LANES), F32)

    def subtract(j, first, count):
        span = pl.ds(pl.multiple_of(first * rows, 16), count * rows)
        three = [src[span, :].astype(F32) for src in (p, o, c)]
        for q in range(count):
            into = pl.ds((first + q - j * LANES) * pitch, rows)
            normal = three[2][q * rows : (q + 1) * rows]
            for a in range(2):
                nat[j][a, into, :] = three[a][q * rows : (q + 1) * rows] - normal
        for q in range(count):
            for v, r in enumerate((0, rows - 1)):
                at = q * rows + r
                f, t, n = (x[at : at + 1, :] for x in three)
                edge[v, 0, pl.ds(first + q, 1), :] = f - t
                edge[v, 1, pl.ds(first + q, 1), :] = t - n

    def subtract_chunk(j, lo, hi):
        whole = (hi - lo) // STEP

        def body(i, carry):
            subtract(j, lo + i * STEP, STEP)
            return carry

        lax.fori_loop(0, whole, body, 0)

        def pair(i, carry):
            subtract(j, lo + whole * STEP + 2 * i, 2)
            return carry

        if lo + whole * STEP < hi:
            lax.fori_loop(0, (hi - lo - whole * STEP) // 2, pair, 0)

    def turn(j, r):
        for a in range(2):
            t = nat[j][a, pl.ds(r, LANES, stride=pitch), :]
            slab[j][a, r, pl.ds(8, LANES), :] = t.T

    for k, (lo, hi) in enumerate(bounds):
        if lo >= LANES:
            break
        for copy in loads[k]:
            copy.wait()

        subtract_chunk(0, lo, hi)

    def turn_rows(lo, hi):
        for r in range(lo, hi):
            turn(0, r)

    turn_rows(0, rows // 2)
    for k, (lo, hi) in enumerate(bounds):
        if lo >= LANES:
            for copy in loads[k]:
                copy.wait()
            subtract_chunk(1, lo, hi)

    for v in range(2):
        for n in range(2):
            edge_out[v, n] = edge[v, n].astype(jnp.bfloat16)
    pl.semaphore_wait(barrier, len(greeted))
    lat_copies = []
    for v, peer in enumerate((up, down)):
        copy = pltpu.make_async_remote_copy(
            src_ref=edge_out.at[v],
            dst_ref=edge_in.at[1 - v],
            send_sem=lat_send.at[v],
            recv_sem=lat_recv.at[1 - v],
            device_id=(peer, lon),
            device_id_type=MESH,
        )
        copy.start()
        lat_copies.append(copy)
    turn_rows(rows // 2, rows)

    def send_columns(j):
        copies = []
        for s, peer in enumerate((left, right)):
            column = 8 if s == 0 else 7 + LANES
            for a in range(2):
                side_out[j, s, :, a, :] = slab[j][a, :, column, :]
        for s, peer in enumerate((left, right)):
            copies.append(
                pltpu.make_async_remote_copy(
                    src_ref=side_out.at[j, s],
                    dst_ref=side_in.at[j, 1 - s, pl.ds(1, rows)],
                    send_sem=lon_send.at[j, s],
                    recv_sem=lon_recv.at[j, 1 - s],
                    device_id=(lat, peer),
                    device_id_type=MESH,
                )
            )
        for n, peer in enumerate(corners):
            v, s = n // 2, n % 2
            copies.append(
                pltpu.make_async_remote_copy(
                    src_ref=side_out.at[j, s, 0 if v == 0 else rows - 1],
                    dst_ref=side_in.at[j, 1 - s, rows + 1 if v == 0 else 0],
                    send_sem=cor_send.at[j, n],
                    recv_sem=cor_recv.at[j, 3 - n],
                    device_id=peer,
                    device_id_type=MESH,
                )
            )
        for copy in copies:
            copy.start()
        return copies[:2], copies[2:]

    def take_columns(j):
        for s, column in enumerate((7, 8 + LANES)):
            for a in range(2):
                slab[j][a, :, column, :] = side_in[j, s, pl.ds(1, rows), a, :]

    def across(ref, index, g):
        low = ref[(*index, pl.ds(g * 8 + 7, 8), slice(None))]
        mid = ref[(*index, pl.ds(pl.multiple_of(g * 8 + 8, 8), 8), slice(None))]
        high = ref[(*index, pl.ds(g * 8 + 9, 8), slice(None))]
        return low + mid + high

    def account(acc, j, r, g, fcst, true):
        s0, s1, s2, s3, s4, s5 = acc
        w = weight[r]
        delta = fcst - true
        diff[j, r, pl.ds(pl.multiple_of(g * 8, 8), 8), :] = delta
        wf = w * fcst
        wt = w * true
        return (
            s0 + (w * delta) * delta,
            s1 + wf,
            s2 + wt,
            s3 + wf * fcst,
            s4 + wt * true,
            s5 + wf * true,
        )

    def inner(j, g, acc):
        fa, ta = across(slab[j], (0, 0), g), across(slab[j], (1, 0), g)
        fb, tb = across(slab[j], (0, 1), g), across(slab[j], (1, 1), g)
        at = pl.ds(pl.multiple_of(g * 8, 8), 8)
        pairs[0, 0, j, at, :], pairs[0, 1, j, at, :] = fa + fb, ta + tb
        for r in range(1, rows - 1):
            fc, tc = across(slab[j], (0, r + 1), g), across(slab[j], (1, r + 1), g)
            acc = account(acc, j, r, g, fa + fb + fc, ta + tb + tc)
            fa, fb, ta, tb = fb, fc, tb, tc
        pairs[1, 0, j, at, :], pairs[1, 1, j, at, :] = fa + fb, ta + tb
        return acc

    def outer(j, g, acc):
        at = pl.ds(pl.multiple_of(g * 8, 8), 8)
        for v, (r, inside, scale) in enumerate(
            ((0, north_in, north), (rows - 1, south_in, south))
        ):
            both = [
                (across(halo, (v, a, j), g) * inside + pairs[v, a, j, at, :]) * scale
                for a in range(2)
            ]
            acc = account(acc, j, r, g, *both)
        return acc

    groups = LANES // 8
    zero = tuple(jnp.zeros((8, LANES), F32) for _ in range(6))
    share = pl.cdiv(rows, groups - 2)

    def mixed(i, acc):
        for q in range(AT_ONCE):
            acc = inner(0, i * AT_ONCE + q + 1, acc)
        for k in range(AT_ONCE * share):
            turn(1, jnp.minimum(i * (AT_ONCE * share) + k, rows - 1))
        return acc

    accs = [None, None]
    lon_copies, cor_copies = [None, None], [None, None]
    lon_copies[0], cor_copies[0] = send_columns(0)
    accs[0] = lax.fori_loop(0, (groups - 2) // AT_ONCE, mixed, zero)
    lon_copies[1], cor_copies[1] = send_columns(1)
    accs[1] = lax.fori_loop(1, groups - 1, lambda g, acc: inner(1, g, acc), zero)

    def side_groups(j, acc):
        for copy in lon_copies[j]:
            copy.wait_recv()
        take_columns(j)
        return lax.fori_loop(
            0, 2, lambda g, acc: inner(j, g * (groups - 1), acc), acc
        )

    accs[0] = side_groups(0, accs[0])
    for copy in lat_copies:
        copy.wait_recv()
    tail = edge_in.shape[2] - LANES
    for v in range(2):
        true = edge_in[v, 1].astype(F32)
        for a, t in enumerate((edge_in[v, 0].astype(F32) + true, true)):
            t = jnp.concatenate([t, jnp.zeros((LANES - tail, LANES), F32)], axis=0)
            for j in range(tiles):
                halo[v, a, j, pl.ds(8, LANES), :] = t[j * LANES : (j + 1) * LANES, :].T
    for j in range(tiles):

        def outer_seven(i, acc, j=j):
            for q in range(7):
                acc = outer(j, i * 7 + q + 1, acc)
            return acc

        accs[j] = lax.fori_loop(0, (groups - 2) // 7, outer_seven, accs[j])
    accs[1] = side_groups(1, accs[1])
    for j in range(tiles):
        for copy in cor_copies[j]:
            copy.wait_recv()
        for s, column in enumerate((7, 8 + LANES)):
            for v, r in enumerate((0, rows + 1)):
                for a in range(2):
                    halo[v, a, j, pl.ds(column, 1), :] = side_in[j, s, r, pl.ds(a, 1), :]
        for g in (0, groups - 1):
            accs[j] = outer(j, g + nought, accs[j])

    for j in range(tiles):
        for n in range(6):
            sums[0, pl.ds(n * tiles + j, 1), :] = jnp.sum(accs[j][n], axis=0, keepdims=True)

    def exchange(stage, me, peers):
        def copy_of(k, slot):
            return pltpu.make_async_remote_copy(
                src_ref=sums.at[stage],
                dst_ref=got.at[stage, slot],
                send_sem=red_send.at[stage, k],
                recv_sem=red_recv.at[stage, slot],
                device_id=peers[k][0],
                device_id_type=MESH,
            )

        for k in range(len(peers)):
            copy_of(k, me).start()
        got[stage, me] = sums[stage]

        def arrive():
            for k, (_, who) in enumerate(peers):
                copy_of(k, who).wait_recv()

        def drain():
            for k in range(len(peers)):
                copy_of(k, me).wait_send()

        return arrive, drain

    def added(stage, count):
        x = got[stage, 0]
        for k in range(1, count):
            x = x + got[stage, k]
        return x

    arrive0, drain0 = exchange(0, z * 2 + core, line_peers)

    def turn_back(r, carry):
        for j in range(tiles):
            t = diff[j, r] * (1.0 / 9.0)
            nat[j][0, pl.ds(r, LANES, stride=pitch), :] = t.T
        return carry

    lax.fori_loop(0, rows // 2, turn_back, 0)
    arrive0()
    sums[1] = added(0, len(line_peers) + 1)
    arrive1, drain1 = exchange(1, x * 4 + y, plane_peers)
    lax.fori_loop(rows // 2, rows, turn_back, 0)

    for j in range(tiles):
        first, count = j * LANES, min(LANES, fields - j * LANES)

        def narrow(i, carry, j=j, first=first):
            for q in range(2):
                f = 2 * i + q
                out_ref[pl.ds(pl.multiple_of((first + f) * rows, 8), rows), :] = nat[j][
                    0, pl.ds(f * pitch, rows), :
                ].astype(jnp.bfloat16)
            return carry

        lax.fori_loop(0, count // 2, narrow, 0)
    for copy in lat_copies + sum(lon_copies + cor_copies, []):
        copy.wait_send()
    drain0()
    drain1()
    arrive1()
    tot_ref[...] = added(1, len(plane_peers) + 1)


def finish(cells, fields, map_ref, tot_ref, out_hbm, rmse_hbm, acc_hbm, rmse_ref, acc_ref, sem):
    tiles = 2
    epsilon = 1e-06
    copy = pltpu.make_async_copy(map_ref, out_hbm, sem.at[0])
    copy.start()
    s = [tot_ref[pl.ds(n * tiles, tiles), :] for n in range(6)]
    one, two = 1.0 / (9.0 * cells), 1.0 / (81.0 * cells)
    mf, mt = s[1] * one, s[2] * one
    vf = s[3] * two - mf * mf
    vt = s[4] * two - mt * mt
    cv = s[5] * two - mf * mt
    rmse = jnp.sqrt(s[0] * two)
    acc = cv / jnp.sqrt((vf + epsilon) * (vt + epsilon))
    for j in range(tiles):
        width_j = min(LANES, fields - j * LANES)
        span = pl.ds(j * LANES, width_j)
        rmse_ref[span] = rmse[j, :width_j]
        acc_ref[span] = acc[j, :width_j]
    small = [
        pltpu.make_async_copy(rmse_ref, rmse_hbm, sem.at[1]),
        pltpu.make_async_copy(acc_ref, acc_hbm, sem.at[2]),
    ]
    for other in small:
        other.start()
    for other in [copy, *small]:
        other.wait()


def local(nlat, nlon, predicted_state, observed_state, longterm_average_state):
    fields, rows, columns = predicted_state.shape
    tiles = pl.cdiv(fields, LANES)
    assert tiles == 2 and fields % 2 == 0
    flat = [
        x.reshape(fields * rows, columns)
        for x in (predicted_state, observed_state, longterm_average_state)
    ]
    edges = list(range(0, fields, CHUNK)) + [fields]
    bounds = tuple(zip(edges[:-1], edges[1:]))
    field_rows = pl.cdiv(fields, 16) * 16
    group = max(nlat, nlon)
    in_vmem = pltpu.VMEM((fields * rows, columns), jnp.bfloat16)
    blurred, totals = pl.pallas_call(
        functools.partial(kernel, nlat, nlon, fields, rows, bounds),
        out_shape=(
            jax.ShapeDtypeStruct((fields * rows, columns), jnp.bfloat16),
            jax.ShapeDtypeStruct((6 * tiles, LANES), F32),
        ),
        in_specs=[pl.BlockSpec(memory_space=pltpu.HBM)] * 3,
        out_specs=[pl.BlockSpec(memory_space=pltpu.VMEM)] * 2,
        scratch_shapes=[
            in_vmem, in_vmem, in_vmem,
            pltpu.VMEM((2, LANES * (rows + 1), LANES), F32),
            pltpu.VMEM((2, LANES * (rows + 1), LANES), F32),
            pltpu.VMEM((2, rows, LANES + 16, LANES), F32),
            pltpu.VMEM((2, rows, LANES + 16, LANES), F32),
            pltpu.VMEM((tiles, rows, LANES, LANES), F32),
            pltpu.VMEM((2, 2, tiles, LANES + 16, LANES), F32),
            pltpu.VMEM((2, 2, field_rows, LANES), F32),
            pltpu.VMEM((2, 2, field_rows, LANES), jnp.bfloat16),
            pltpu.VMEM((2, 2, field_rows, LANES), jnp.bfloat16),
            pltpu.VMEM((tiles, 2, rows, 2, LANES), F32),
            pltpu.VMEM((tiles, 2, rows + 2, 2, LANES), F32),
            pltpu.VMEM((2, 2, tiles, LANES, LANES), F32),
            pltpu.VMEM((rows, 8, LANES), F32),
            pltpu.VMEM((2, 6 * tiles, LANES), F32),
            pltpu.VMEM((2, group, 6 * tiles, LANES), F32),
            pltpu.SemaphoreType.DMA((len(bounds), 3)),
            pltpu.SemaphoreType.DMA((2,)),
            pltpu.SemaphoreType.DMA((2,)),
            pltpu.SemaphoreType.DMA((tiles, 2)),
            pltpu.SemaphoreType.DMA((tiles, 2)),
            pltpu.SemaphoreType.DMA((tiles, 4)),
            pltpu.SemaphoreType.DMA((tiles, 4)),
            pltpu.SemaphoreType.DMA((2, group)),
            pltpu.SemaphoreType.DMA((2, group)),
        ],
        compiler_params=pltpu.CompilerParams(
            collective_id=0, has_side_effects=True, vmem_limit_bytes=50 * 1024 * 1024
        ),
    )(*flat)
    blurred, rmse, acc = pl.pallas_call(
        functools.partial(finish, float(nlat * rows * nlon * columns), fields),
        out_shape=(
            jax.ShapeDtypeStruct((fields * rows, columns), jnp.bfloat16),
            jax.ShapeDtypeStruct((fields,), F32),
            jax.ShapeDtypeStruct((fields,), F32),
        ),
        in_specs=[pl.BlockSpec(memory_space=pltpu.VMEM)] * 2,
        out_specs=[pl.BlockSpec(memory_space=pltpu.HBM)] * 3,
        scratch_shapes=[
            pltpu.VMEM((fields,), F32),
            pltpu.VMEM((fields,), F32),
            pltpu.SemaphoreType.DMA((3,)),
        ],
        compiler_params=pltpu.CompilerParams(vmem_limit_bytes=8 * 1024 * 1024),
    )(blurred, totals)
    return (
        blurred.reshape(fields, rows, columns),
        rmse,
        acc,
    )


def solution(mesh):
    placed = (P(None, "lat", "lon"), P(None, "lat", "lon"), P(None, "lat", "lon"))
    return jax.shard_map(
        functools.partial(local, mesh.shape["lat"], mesh.shape["lon"]),
        mesh=mesh,
        in_specs=placed,
        out_specs=(P(None, "lat", "lon"), P(), P()),
        check_vma=False,
    )
```
